32 devices in a mesh: expert: 8 (over z, core), latent: 2 (over y), row: 2 (over x).
Axes of the slice: x: 2, y: 2, z: 4, core: 2. Of those that a mesh axis runs over, the one named last changes fastest.
Arguments:
- model_acts: bfloat16 [512, 8192], P('row', 'expert'), may hold values from -6 to 6
- enc_weight: bfloat16 [8192, 12288], P('expert', ('latent', 'row')), may hold values from -0.0625 to 0.0625
- dec_weight: bfloat16 [12288, 8192], P(('latent', 'row'), 'expert'), may hold values from -0.0546875 to 0.0546875
- enc_bias: float32 [12288], P('latent'), may hold values from -3 to 3
- dec_bias: float32 [8192], P('expert'), may hold values from -3 to 3
- enc_first: bfloat16 [8192, 12288], P('expert', ('latent', 'row')), may hold values from -0.119628906 to 0.119628906
- enc_second: bfloat16 [8192, 12288], P('expert', ('latent', 'row')), may hold values from 9.9658966e-05 to 0.0099487305
- dec_first: bfloat16 [12288, 8192], P(('latent', 'row'), 'expert'), may hold values from -0.119628906 to 0.119628906
- dec_second: bfloat16 [12288, 8192], P(('latent', 'row'), 'expert'), may hold values from 9.9658966e-05 to 0.0099487305
Outputs:
- encoder_next: bfloat16 [8192, 12288], P('expert', ('latent', 'row'))
- decoder_next: bfloat16 [12288, 8192], P(('latent', 'row'), 'expert')
- enc_first_next: bfloat16 [8192, 12288], P('expert', ('latent', 'row'))
- enc_second_next: bfloat16 [8192, 12288], P('expert', ('latent', 'row'))
- dec_first_next: bfloat16 [12288, 8192], P(('latent', 'row'), 'expert')
- dec_second_next: bfloat16 [12288, 8192], P(('latent', 'row'), 'expert')
- enc_bias_grad: float32 [12288], P(('latent', 'row'))
- dec_bias_grad: float32 [8192], P('expert')
The draws below stay inside these ranges and needn't reach their ends.
All inputs are finite; a program needn't handle non-finite values.
Results may differ from the reference program's by a relative error of at most 0.005.
Values may be sent and summed in bfloat16 or wider, within the bound.
No kernel may reach another device: no remote copies, remote signals or barrier semaphores. Data moves between devices by JAX's collectives and lax.ppermute only.
A program may use at most 128 MiB of HBM per device.

```python
import math
import jax
import jax.numpy as jnp
from jax import lax

EXPERTS = 8
D = 1024
L = 12288
ROWS = 512


def steps_of(own_key, extent, split, least, high):
    gain = 1.0
    for dim, blocks in split:
        draws = jax.random.uniform(jax.random.fold_in(jax.random.fold_in(own_key, 6), dim), (blocks,), jnp.float32, least / len(split), high / len(split))
        gain = gain * jnp.repeat(jnp.exp(draws), extent[dim] // blocks).reshape((-1,) + (1,) * (len(extent) - 1 - dim))
    return gain


def bell_draw(own_key, shape, deviation, reach, shards=(), held_as=jnp.bfloat16):
    entries = jax.random.normal(own_key, shape, jnp.float32) * deviation
    if len(shards) > 0:
        entries = steps_of(own_key, shape, shards, -0.22, 0.18) * entries
    return jnp.clip(entries, min=-reach, max=reach).astype(held_as)


def setup_inputs(seed: int = 0) -> dict:
    splits = jax.random.split(jax.random.key(seed), 10)
    model_acts = bell_draw(splits[0], (ROWS, EXPERTS * D), 1.0, 6.0, ((0, 2), (1, 8)))
    enc_weight = bell_draw(splits[1], (EXPERTS * D, L), (EXPERTS * D) ** -0.5, 0.0625, ((0, 8), (1, 4)))
    dec_weight = bell_draw(splits[2], (L, EXPERTS * D), L ** -0.5, 0.0546875, ((0, 4), (1, 8)))
    enc_bias = bell_draw(splits[3], (L,), 0.5, 3.0, ((0, 2),), jnp.float32)
    dec_bias = bell_draw(splits[4], (EXPERTS * D,), 0.5, 3.0, ((0, 8),), jnp.float32)
    enc_first = bell_draw(splits[5], (EXPERTS * D, L), 0.02, 0.119628906, ((0, 8), (1, 4)))
    enc_second = jnp.clip(jnp.exp(math.log(0.0099487305) - 4.603446 * jax.random.uniform(splits[6], (EXPERTS * D, L), jnp.float32) ** steps_of(splits[6], (EXPERTS * D, L), ((0, 8), (1, 4)), -0.2, 0.2)), 9.965896606445312e-05, 0.0099487305).astype(jnp.bfloat16)
    dec_first = bell_draw(splits[7], (L, EXPERTS * D), 0.02, 0.119628906, ((0, 4), (1, 8)))
    dec_second = jnp.clip(jnp.exp(math.log(0.0099487305) - 4.603446 * jax.random.uniform(splits[8], (L, EXPERTS * D), jnp.float32) ** steps_of(splits[8], (L, EXPERTS * D), ((0, 4), (1, 8)), -0.2, 0.2)), 9.965896606445312e-05, 0.0099487305).astype(jnp.bfloat16)
    return {"model_acts": model_acts, "enc_weight": enc_weight, "dec_weight": dec_weight, "enc_bias": enc_bias, "dec_bias": dec_bias, "enc_first": enc_first, "enc_second": enc_second, "dec_first": dec_first, "dec_second": dec_second}


beta_one = 0.9
beta_two = 0.999
learn_rate = 0.001
adam_eps = 1e-08
bias_one = 0.9999734386011124
bias_two = 0.09520785288629115
norm_eps = 1e-06
sparsity = 1.0

def adam_step(weight, moment_one, moment_two, gradient):
    first_next = beta_one * moment_one.astype(jnp.float32) + (1.0 - beta_one) * gradient
    second_next = beta_two * moment_two.astype(jnp.float32) + (1.0 - beta_two) * gradient * gradient
    stepped = weight.astype(jnp.float32) - learn_rate * (first_next / bias_one) / (jnp.sqrt(second_next / bias_two) + adam_eps)
    return (stepped.astype(jnp.bfloat16), first_next.astype(jnp.bfloat16), second_next.astype(jnp.bfloat16))

def reference(model_acts, enc_weight, dec_weight, enc_bias, dec_bias, enc_first, enc_second, dec_first, dec_second):
    total_rows = model_acts.shape[0]
    preact = jnp.dot(model_acts, enc_weight, preferred_element_type=jnp.float32) + enc_bias
    latent_low = jnp.maximum(preact, 0.0).astype(jnp.bfloat16)
    rebuilt = jnp.dot(latent_low, dec_weight, preferred_element_type=jnp.float32) + dec_bias
    grad_rows = 2.0 * (rebuilt - model_acts.astype(jnp.float32)) / total_rows
    grad_low = grad_rows.astype(jnp.bfloat16)
    decoder_wide = dec_weight.astype(jnp.float32).reshape(L, EXPERTS, D)
    decoder_norms = jnp.sqrt(lax.optimization_barrier(jnp.sum(decoder_wide * decoder_wide, axis=2)) + norm_eps)
    strength = lax.optimization_barrier(jnp.sum(decoder_norms, axis=1))
    col_total = lax.optimization_barrier(jnp.sum(latent_low.astype(jnp.float32), axis=0)) / total_rows
    dec_grad = jnp.dot(latent_low.T, grad_low, preferred_element_type=jnp.float32)
    dec_grad = dec_grad + sparsity * col_total[:, None] * (decoder_wide / decoder_norms[:, :, None]).reshape(L, EXPERTS * D)
    dec_bias_grad = lax.optimization_barrier(jnp.sum(grad_rows, axis=0))
    back_grad = jnp.dot(grad_low, dec_weight.T, preferred_element_type=jnp.float32) + sparsity * strength / total_rows
    grad_pre = jnp.where(preact > 0, back_grad, 0.0).astype(jnp.bfloat16)
    enc_grad = jnp.dot(model_acts.T, grad_pre, preferred_element_type=jnp.float32)
    enc_bias_grad = lax.optimization_barrier(jnp.sum(grad_pre.astype(jnp.float32), axis=0))
    encoder_next, enc_first_next, enc_second_next = adam_step(enc_weight, enc_first, enc_second, enc_grad)
    decoder_next, dec_first_next, dec_second_next = adam_step(dec_weight, dec_first, dec_second, dec_grad)
    return (encoder_next, decoder_next, enc_first_next, enc_second_next, dec_first_next, dec_second_next, enc_bias_grad, dec_bias_grad)
```

```python
import functools

import jax
import jax.numpy as jnp
from jax import lax
from jax.experimental import pallas as pl
from jax.experimental.pallas import tpu as pltpu
from jax.sharding import Mesh, PartitionSpec as P

D = 1024
GROUPS = 2
PIECES = 6
LANES = 128
VMEM_LIMIT = 24 * 2**20


beta_one = 0.9
beta_two = 0.999
learn_rate = 0.001
adam_eps = 1e-08
bias_one = 0.9999734386011124
bias_two = 0.09520785288629115
norm_eps = 1e-06
sparsity = 1.0

f32 = jnp.float32
bf16 = jnp.bfloat16


def adam_kernel(groups, decays, *refs):
    lefts, rights, refs = refs[:groups], refs[groups : 2 * groups], refs[2 * groups :]
    turned, refs = refs[-groups:], refs[:-groups]
    weight_ref, first_ref, second_ref = refs[:3]
    weight_out, first_out, second_out = refs[-3:]
    gradient = None
    for left, right, across in zip(lefts, rights, turned):
        across[...] = left[...].T
        part = jnp.dot(across[...], right[...], preferred_element_type=f32)
        gradient = part if gradient is None else gradient + part
    weight = weight_ref[...].astype(f32)
    if decays:
        scale = jnp.concatenate([refs[3][...]] * (weight.shape[1] // LANES), axis=1)
        gradient = gradient + scale * weight
    rate = bias_one / learn_rate
    tenth = (1.0 - beta_one) * gradient
    first_next = beta_one * first_ref[...].astype(f32) + tenth
    second_next = beta_two * second_ref[...].astype(f32) + (
        (1.0 - beta_two) / (1.0 - beta_one) ** 2 * (tenth * tenth)
    )
    square = second_next * (rate * rate / bias_two)
    stepped = weight - first_next / (square * lax.rsqrt(square) + rate * adam_eps)
    weight_out[...] = stepped.astype(bf16)
    first_out[...] = first_next.astype(bf16)
    second_out[...] = second_next.astype(bf16)


def adam_rows(lefts, rights, weight, first, second, tile, scale=None, done=None, begin=0, end=None):
    height, width = weight.shape
    end = height if end is None else end
    depth = lefts[0].shape[0]
    skip = begin // tile
    state = pl.BlockSpec((tile, width), lambda i: (i + skip, 0))
    in_specs = [pl.BlockSpec((depth, tile), lambda i: (0, i + skip))] * len(lefts)
    in_specs += [pl.BlockSpec((depth, width), lambda i: (0, 0))] * len(rights)
    in_specs += [state] * 3
    operands = [*lefts, *rights, weight, first, second]
    if scale is not None:
        in_specs.append(pl.BlockSpec((tile, LANES), lambda i: (i + skip, 0)))
        operands.append(scale)
    kernel = functools.partial(adam_kernel, len(lefts), scale is not None)
    aliases = {}
    if done is not None:
        fixed, inner = len(operands), kernel
        aliases = {fixed + i: i for i in range(3)}
        in_specs += [pl.BlockSpec(memory_space=pl.ANY)] * 3
        operands += done

        def kernel(*refs):
            inner(*refs[:fixed], *refs[fixed + 3 :])

    part = end - begin
    return pl.pallas_call(
        kernel,
        grid=(part // tile,),
        in_specs=in_specs,
        out_specs=[state] * 3,
        out_shape=[jax.ShapeDtypeStruct(weight.shape, bf16)] * 3,
        scratch_shapes=[pltpu.VMEM((tile, depth), bf16)] * len(lefts),
        input_output_aliases=aliases,
        cost_estimate=pl.CostEstimate(
            flops=2 * part * width * depth * len(lefts),
            bytes_accessed=12 * part * width,
            transcendentals=2 * part * width,
        ),
        compiler_params=pltpu.CompilerParams(vmem_limit_bytes=VMEM_LIMIT),
        name="adam",
    )(*operands)


def after(value, earlier):
    return value if earlier is None else lax.optimization_barrier((value, earlier))[0]


class Moves:
    def __init__(self, chips, latents, rows):
        self.chips, self.latents, self.rows = chips, latents, rows

    def sibling(self, value):
        return lax.ppermute(value, "core", [(0, 1), (1, 0)])

    def hop(self, value, first, last):
        top = self.chips - 1
        pairs = []
        for place in range(first, last + 1):
            pairs.append((place * 2, (place + 1) * 2))
            pairs.append(((top - place) * 2 + 1, (top - place - 1) * 2 + 1))
        return lax.ppermute(value, ("z", "core"), pairs)

    def flipped(self, blocks):
        return jnp.concatenate([blocks[:1], blocks[1:][::-1]], axis=0)

    def reduce_own(self, blocks, other, wire, earlier):
        other = self.flipped(other)
        carried = None
        for step in range(1, self.chips):
            part = blocks[step].astype(f32) + other[step].astype(f32)
            if carried is not None:
                part = part + carried.astype(f32)
            carried = self.hop(part.astype(wire), 0, step - 1)
        here = blocks[0].astype(f32) + other[0].astype(f32)
        away = after(self.sibling(carried), earlier)
        return here + (carried.astype(f32) + away.astype(f32))

    def gather_own(self, block):
        got, carried = [], block
        for step in range(1, self.chips):
            carried = self.hop(carried, step - 1, self.chips - 2)
            got.append(carried)
        got = jnp.stack(got)
        return jnp.concatenate([block[None], got + self.sibling(got)[::-1]], axis=0)

    def partner(self, value, step):
        axes = [("row", 1)]
        bit = 1
        while bit < self.latents:
            axes.append(("latent", bit))
            bit *= 2
        pairs = []
        for core, (axis, mask) in enumerate((axes[step], axes[len(axes) - 1 - step])):
            for latent in range(self.latents):
                for row in range(self.rows):
                    to = (latent ^ mask, row) if axis == "latent" else (latent, row ^ mask)
                    pairs.append(
                        (
                            (core * self.latents + latent) * self.rows + row,
                            (core * self.latents + to[0]) * self.rows + to[1],
                        )
                    )
        return lax.ppermute(value, ("core", "latent", "row"), pairs)

    def reduce_latents(self, part):
        steps = 1 + (self.latents.bit_length() - 1)
        total = part
        for step in range(steps):
            sent = total.astype(bf16)
            total = sent.astype(f32) + self.partner(sent, step).astype(f32)
        return total


def local(
    moves,
    model_acts,
    enc_weight,
    dec_weight,
    enc_bias,
    dec_bias,
    enc_first,
    enc_second,
    dec_first,
    dec_second,
):
    local_rows, shard_width = model_acts.shape
    local_latents = enc_weight.shape[1]
    chips = moves.chips
    total_rows = local_rows * moves.rows
    core, place, row_index = lax.axis_index("core"), lax.axis_index("z"), lax.axis_index("row")
    shards_per_expert = D // shard_width
    sub = local_rows // (GROUPS * chips)
    block_rows = sub * moves.rows

    bias_here = lax.dynamic_slice_in_dim(enc_bias, row_index * local_latents, local_latents)

    turned = model_acts.reshape(GROUPS, chips, sub, shard_width)
    step_of = jnp.where(core == 0, -jnp.arange(chips), jnp.arange(chips))
    turned = jnp.take(turned, (place + step_of) % chips, axis=1)

    tokens = []
    for group in range(GROUPS):
        own = turned[group]
        away = after(lax.ppermute(own, "row", [(0, 1), (1, 0)]), tokens[-1] if tokens else None)
        first, second = jnp.where(row_index == 0, own, away), jnp.where(row_index == 0, away, own)
        tokens.append(jnp.concatenate([first, second], axis=1).reshape(chips * block_rows, shard_width))

    wide = dec_weight.astype(f32)
    partial_sq = jnp.sum(wide * wide, axis=1)
    if shards_per_expert > 1:
        partial_sq = partial_sq + moves.sibling(partial_sq)
    own_norm = jnp.sqrt(partial_sq + norm_eps)
    penalty = sparsity * own_norm / (total_rows * shards_per_expert)

    lat, low, pre, col_total, row_bias, bias_sum = [], [], [], 0.0, 0.0, 0.0
    first_block = second_block = grad_low = None
    for group in range(GROUPS):
        part = jnp.dot(tokens[group], enc_weight, preferred_element_type=f32)
        part = part.reshape(chips, block_rows, local_latents)
        preact = moves.reduce_own(part, moves.sibling(part), f32, first_block) + bias_here
        active = preact > 0
        first_block = jnp.maximum(preact, 0.0).astype(bf16)
        latent = moves.gather_own(first_block)
        latent = latent.reshape(chips * block_rows, local_latents)
        rebuilt = jnp.dot(latent, dec_weight, preferred_element_type=f32)
        rebuilt = after(moves.reduce_latents(rebuilt), grad_low)
        grad_rows = 2.0 * (rebuilt + dec_bias - tokens[group].astype(f32)) / total_rows
        grad_low = grad_rows.astype(bf16)
        back = lax.dot_general(
            grad_low, dec_weight, (((1,), (1,)), ((), ())), preferred_element_type=f32
        )
        back = (back + penalty).astype(bf16).reshape(chips, block_rows, local_latents)
        back_grad = moves.reduce_own(back, moves.sibling(back), bf16, second_block)
        second_block = jnp.where(active, back_grad, 0.0).astype(bf16)
        grad_pre = moves.gather_own(second_block)
        grad_pre = grad_pre.reshape(chips * block_rows, local_latents)
        lat.append(latent)
        low.append(grad_low)
        pre.append(grad_pre)
        col_total = col_total + jnp.sum(latent.astype(f32), axis=0)
        row_bias = row_bias + jnp.sum(grad_rows, axis=0)
        bias_sum = bias_sum + jnp.sum(grad_pre.astype(f32), axis=0)

    scale = sparsity * col_total / (total_rows * own_norm)
    scale = jnp.broadcast_to(scale[:, None], (local_latents, LANES))
    piece_rows = local_latents // PIECES
    tile = 2 * LANES if piece_rows % (2 * LANES) == 0 else LANES
    done = None
    for piece in range(PIECES):
        begin = piece * piece_rows
        done = adam_rows(
            lat, low, dec_weight, dec_first, dec_second, tile, scale, done, begin, begin + piece_rows
        )
    decoder_next, dec_first_next, dec_second_next = done
    encoder_next, enc_first_next, enc_second_next = adam_rows(
        tokens, pre, enc_weight, enc_first, enc_second, LANES
    )
    return (
        encoder_next,
        decoder_next,
        enc_first_next,
        enc_second_next,
        dec_first_next,
        dec_second_next,
        bias_sum,
        row_bias,
    )


def solution(mesh):
    experts, latents, rows = (mesh.shape[name] for name in ("expert", "latent", "row"))
    fine = Mesh(
        mesh.devices.reshape(experts // 2, 2, latents, rows), ("z", "core", "latent", "row")
    )
    moves = Moves(experts // 2, latents, rows)
    expert = ("z", "core")
    enc, dec = P(expert, ("latent", "row")), P(("latent", "row"), expert)

    def body(*arrays):
        return local(moves, *arrays)

    return jax.shard_map(
        body,
        mesh=fine,
        in_specs=(P("row", expert), enc, dec, P("latent"), P(expert), enc, enc, dec, dec),
        out_specs=(enc, dec, enc, enc, dec, dec, P(("latent", "row")), P(expert)),
        check_vma=False,
    )
```

```python
import functools

import jax
import jax.numpy as jnp
from jax import lax
from jax.experimental import pallas as pl
from jax.experimental.pallas import tpu as pltpu
from jax.sharding import Mesh, PartitionSpec as P

D = 1024
GROUPS = 2
PIECES = 6
LANES = 128
ENC_LIMIT = 36 * 2**20


beta_one = 0.9
beta_two = 0.999
learn_rate = 0.001
adam_eps = 1e-08
bias_one = 0.9999734386011124
bias_two = 0.09520785288629115
norm_eps = 1e-06
sparsity = 1.0

f32 = jnp.float32
bf16 = jnp.bfloat16


def adam_kernel(groups, decays, *refs):
    lefts, rights, refs = refs[:groups], refs[groups : 2 * groups], refs[2 * groups :]
    turned, refs = refs[-groups:], refs[:-groups]
    weight_ref, first_ref, second_ref = refs[:3]
    weight_out, first_out, second_out = refs[-3:]
    gradient = None
    for left, right, across in zip(lefts, rights, turned):
        across[...] = left[...].T
        part = jnp.dot(across[...], right[...], preferred_element_type=f32)
        gradient = part if gradient is None else gradient + part
    weight = weight_ref[...].astype(f32)
    if decays:
        scale = jnp.concatenate([refs[3][...]] * (weight.shape[1] // LANES), axis=1)
        gradient = gradient + scale * weight
    rate = bias_one / learn_rate
    tenth = (1.0 - beta_one) * gradient
    first_next = beta_one * first_ref[...].astype(f32) + tenth
    second_next = beta_two * second_ref[...].astype(f32) + (
        (1.0 - beta_two) / (1.0 - beta_one) ** 2 * (tenth * tenth)
    )
    square = second_next * (rate * rate / bias_two)
    stepped = weight - first_next / (square * lax.rsqrt(square) + rate * adam_eps)
    weight_out[...] = stepped.astype(bf16)
    first_out[...] = first_next.astype(bf16)
    second_out[...] = second_next.astype(bf16)


def adam_rows(lefts, rights, weight, first, second, tile, limit, scale=None, done=None, begin=0, end=None):
    height, width = weight.shape
    end = height if end is None else end
    depth = lefts[0].shape[0]
    skip = begin // tile
    state = pl.BlockSpec((tile, width), lambda i: (i + skip, 0))
    in_specs = [pl.BlockSpec((depth, tile), lambda i: (0, i + skip))] * len(lefts)
    in_specs += [pl.BlockSpec((depth, width), lambda i: (0, 0))] * len(rights)
    in_specs += [state] * 3
    operands = [*lefts, *rights, weight, first, second]
    if scale is not None:
        in_specs.append(pl.BlockSpec((tile, LANES), lambda i: (i + skip, 0)))
        operands.append(scale)
    kernel = functools.partial(adam_kernel, len(lefts), scale is not None)
    aliases = {}
    if done is not None:
        fixed, inner = len(operands), kernel
        aliases = {fixed + i: i for i in range(3)}
        in_specs += [pl.BlockSpec(memory_space=pl.ANY)] * 3
        operands += done

        def kernel(*refs):
            inner(*refs[:fixed], *refs[fixed + 3 :])

    part = end - begin
    return pl.pallas_call(
        kernel,
        grid=(part // tile,),
        in_specs=in_specs,
        out_specs=[state] * 3,
        out_shape=[jax.ShapeDtypeStruct(weight.shape, bf16)] * 3,
        scratch_shapes=[pltpu.VMEM((tile, depth), bf16)] * len(lefts),
        input_output_aliases=aliases,
        cost_estimate=pl.CostEstimate(
            flops=2 * part * width * depth * len(lefts),
            bytes_accessed=12 * part * width,
            transcendentals=2 * part * width,
        ),
        compiler_params=pltpu.CompilerParams(vmem_limit_bytes=limit),
        name="adam",
    )(*operands)


def after(value, earlier):
    return value if earlier is None else lax.optimization_barrier((value, earlier))[0]


class Moves:
    def __init__(self, chips, latents, rows):
        self.chips, self.latents, self.rows = chips, latents, rows

    def sibling(self, value):
        return lax.ppermute(value, "core", [(0, 1), (1, 0)])

    def hop(self, value, first, last):
        top = self.chips - 1
        pairs = []
        for place in range(first, last + 1):
            pairs.append((place * 2, (place + 1) * 2))
            pairs.append(((top - place) * 2 + 1, (top - place - 1) * 2 + 1))
        return lax.ppermute(value, ("z", "core"), pairs)

    def reduce_own(self, block, wire, earlier):
        carried = None
        for step in range(1, self.chips):
            part = block(step)
            if carried is not None:
                part = part + carried.astype(f32)
            carried = self.hop(part.astype(wire), 0, step - 1)
        away = after(self.sibling(carried), earlier)
        return block(0) + (carried.astype(f32) + away.astype(f32))

    def gather_own(self, block, earlier):
        got = [block]
        for step in range(1, self.chips):
            got.append(self.hop(got[-1], step - 1, self.chips - 2))
        got[-1] = after(got[-1], earlier)
        sent = jnp.stack([jnp.zeros_like(block), *got[:0:-1]])
        away = self.sibling(sent)
        return jnp.stack(got) + away, sent

    def summed(self, parts, others, row_index):
        sums = lambda t: [part[t].astype(f32) + other[-t].astype(f32) for part, other in zip(parts, others)]

        def block(t):
            found = sums(t)
            if len(found) == 1:
                return found[0]
            own, away = found
            here = row_index == 0
            return jnp.concatenate([jnp.where(here, own, away), jnp.where(here, away, own)])

        return block

    def partner(self, value, step):
        axes = [("row", 1)]
        bit = 1
        while bit < self.latents:
            axes.append(("latent", bit))
            bit *= 2
        pairs = []
        for core, (axis, mask) in enumerate((axes[step], axes[len(axes) - 1 - step])):
            for latent in range(self.latents):
                for row in range(self.rows):
                    to = (latent ^ mask, row) if axis == "latent" else (latent, row ^ mask)
                    pairs.append(
                        (
                            (core * self.latents + latent) * self.rows + row,
                            (core * self.latents + to[0]) * self.rows + to[1],
                        )
                    )
        return lax.ppermute(value, ("core", "latent", "row"), pairs)

    def reduce_latents(self, part, earlier):
        steps = 1 + (self.latents.bit_length() - 1)
        total = part
        for step in range(steps):
            sent = total.astype(bf16)
            got = self.partner(sent, step)
            got = after(got, earlier if step == steps - 1 else None)
            total = sent.astype(f32) + got.astype(f32)
        return total


def local(
    moves,
    model_acts,
    enc_weight,
    dec_weight,
    enc_bias,
    dec_bias,
    enc_first,
    enc_second,
    dec_first,
    dec_second,
):
    local_rows, shard_width = model_acts.shape
    local_latents = enc_weight.shape[1]
    chips = moves.chips
    total_rows = local_rows * moves.rows
    core, place, row_index = lax.axis_index("core"), lax.axis_index("z"), lax.axis_index("row")
    shards_per_expert = D // shard_width
    sub = local_rows // (GROUPS * chips)
    block_rows = sub * moves.rows

    bias_here = lax.dynamic_slice_in_dim(enc_bias, row_index * local_latents, local_latents)

    turned = model_acts.reshape(GROUPS, chips, sub, shard_width)
    step_of = jnp.where(core == 0, -jnp.arange(chips), jnp.arange(chips))
    turned = jnp.take(turned, (place + step_of) % chips, axis=1)

    tokens, halves = [], []
    for group in range(GROUPS):
        own = turned[group]
        away = after(lax.ppermute(own, "row", [(0, 1), (1, 0)]), tokens[-1] if tokens else None)
        first, second = jnp.where(row_index == 0, own, away), jnp.where(row_index == 0, away, own)
        tokens.append(jnp.concatenate([first, second], axis=1).reshape(chips * block_rows, shard_width))
        halves.append((tokens[-1],))

    wide = dec_weight.astype(f32)
    partial_sq = jnp.sum(wide * wide, axis=1)
    if shards_per_expert > 1:
        partial_sq = partial_sq + moves.sibling(partial_sq)
    own_norm = jnp.sqrt(partial_sq + norm_eps)
    penalty = sparsity * own_norm / (total_rows * shards_per_expert)

    lat, low, pre, col_total, row_bias, bias_sum = [], [], [], 0.0, 0.0, 0.0
    first_block = second_block = first_sent = second_sent = grad_low = None
    for group in range(GROUPS):
        parts, others = [], []
        for rows in halves[group]:
            rows = rows.reshape(-1, shard_width)
            part = jnp.dot(rows, enc_weight, preferred_element_type=f32)
            parts.append(part.reshape(chips, -1, local_latents))
            others.append(moves.sibling(parts[-1]))
        block = moves.summed(parts, others, row_index)
        preact = moves.reduce_own(block, f32, first_block) + bias_here
        active = preact > 0
        first_block = jnp.maximum(preact, 0.0).astype(bf16)
        latent, first_sent = moves.gather_own(first_block, first_sent)
        latent = latent.reshape(chips * block_rows, local_latents)
        rebuilt = jnp.dot(latent, dec_weight, preferred_element_type=f32)
        rebuilt = moves.reduce_latents(rebuilt, grad_low)
        grad_rows = 2.0 * (rebuilt + dec_bias - tokens[group].astype(f32)) / total_rows
        grad_low = grad_rows.astype(bf16)
        back = lax.dot_general(
            grad_low, dec_weight, (((1,), (1,)), ((), ())), preferred_element_type=f32
        )
        back = (back + penalty).astype(bf16).reshape(chips, block_rows, local_latents)
        block = moves.summed([back], [moves.sibling(back)], row_index)
        back_grad = moves.reduce_own(block, bf16, second_block)
        second_block = jnp.where(active, back_grad, 0.0).astype(bf16)
        grad_pre, second_sent = moves.gather_own(second_block, second_sent)
        grad_pre = grad_pre.reshape(chips * block_rows, local_latents)
        lat.append(latent)
        low.append(grad_low)
        pre.append(grad_pre)
        col_total = col_total + jnp.sum(latent.astype(f32), axis=0)
        row_bias = row_bias + jnp.sum(grad_rows, axis=0)
        bias_sum = bias_sum + jnp.sum(grad_pre.astype(f32), axis=0)

    scale = sparsity * col_total / (total_rows * own_norm)
    scale = jnp.broadcast_to(scale[:, None], (local_latents, LANES))
    piece_rows = local_latents // PIECES
    tile = 2 * LANES if piece_rows % (2 * LANES) == 0 else LANES
    done = None
    for piece in range(PIECES):
        begin = piece * piece_rows
        done = adam_rows(
            lat, low, dec_weight, dec_first, dec_second, tile, 24 * 2**20, scale, done, begin, begin + piece_rows
        )
    decoder_next, dec_first_next, dec_second_next = done
    encoder_next, enc_first_next, enc_second_next = adam_rows(
        tokens, pre, enc_weight, enc_first, enc_second, LANES, ENC_LIMIT
    )
    return (
        encoder_next,
        decoder_next,
        enc_first_next,
        enc_second_next,
        dec_first_next,
        dec_second_next,
        bias_sum,
        row_bias,
    )


def solution(mesh):
    experts, latents, rows = (mesh.shape[name] for name in ("expert", "latent", "row"))
    fine = Mesh(
        mesh.devices.reshape(experts // 2, 2, latents, rows), ("z", "core", "latent", "row")
    )
    moves = Moves(experts // 2, latents, rows)
    expert = ("z", "core")
    enc, dec = P(expert, ("latent", "row")), P(("latent", "row"), expert)

    def body(*arrays):
        return local(moves, *arrays)

    return jax.shard_map(
        body,
        mesh=fine,
        in_specs=(P("row", expert), enc, dec, P("latent"), P(expert), enc, enc, dec, dec),
        out_specs=(enc, dec, enc, enc, dec, dec, P(("latent", "row")), P(expert)),
        check_vma=False,
    )
```
